256 devices in a mesh: group: 32 (over x, y, core), inst: 8 (over z).
Axes of the slice: x: 4, y: 4, z: 8, core: 2. Of those that a mesh axis runs over, the one named last changes fastest.
Arguments:
- old_cache: bfloat16 [8, 2048, 16, 2048], P('inst', 'group'), may hold values from -64 to 64, as said below
- block_table: int32 [128, 128], replicated, may hold values from 0 to 2047, as said below
- place_after: int32 [128], replicated, may hold values from 0 to 127, as said below
- context_len: int32 [128], replicated, may hold values from 256 to 2048
- queries: bfloat16 [32768, 4096], P(('group', 'inst')), may hold values from -64 to 64
- new_kv: bfloat16 [32768, 2048], P(('group', 'inst')), may hold values from -6 to 6
Outputs:
- attended: bfloat16 [32768, 4096], P(('group', 'inst'))
The draws below stay inside these ranges and needn't reach their ends.
Inputs may be any that keep to these rules, and one draw needn't show every extreme that they name: Each of old_cache and queries lies within the printed range. A permutation: request r moves to group index place_after[r] // 4, as that group's request number place_after[r] % 4. block_table[r, k] lies on the devices of inst index k // 16: on group index block_table[r, k] // 64, slot block_table[r, k] % 64. Every slot of every device holds exactly one block, and each device holds exactly 2 blocks of the requests of each new group.
All inputs are finite; a program needn't handle non-finite values.
Results may differ from the reference program's by a relative error of at most 0.0075.
Values may be sent and summed in bfloat16 or wider, within the bound.
A program may use at most 128 MiB of HBM per device.

```python
import jax
import jax.numpy as jnp
from jax import lax

HQ = 32
KVH = 8
HD = 128
BLK = 16
CTX = 2048
PRE = 256
REQS = 128
NBLK = 128
NBI = 16
N_GROUP = 32
N_INST = 8


def layout_plan(key):
    rgroup = N_INST // 2
    reqs = rgroup * N_GROUP
    nblk = CTX // BLK
    per_inst = nblk // N_INST
    slots = rgroup * per_inst
    per_pair = slots // N_GROUP
    base = jax.random.fold_in(key, 101)
    after = jax.random.permutation(jax.random.fold_in(base, 1), reqs).astype(jnp.int32)
    request_of = jnp.argsort(after).astype(jnp.int32)
    item_keys = jax.random.split(jax.random.fold_in(base, 2), N_INST * N_GROUP)
    items = jax.vmap(lambda k: jax.random.permutation(k, slots))(item_keys).reshape(N_INST, N_GROUP, slots).astype(jnp.int32)
    slot_keys = jax.random.split(jax.random.fold_in(base, 3), N_INST * N_GROUP)
    sigma = jax.vmap(lambda k: jax.random.permutation(k, slots))(slot_keys).reshape(N_INST, N_GROUP, slots).astype(jnp.int32)
    position = jnp.arange(slots, dtype=jnp.int32)
    source = position // per_pair
    target = jnp.arange(N_GROUP, dtype=jnp.int32)
    local_pos = target[:, None] * per_pair + position[None, :] % per_pair
    inst_ids = jnp.arange(N_INST, dtype=jnp.int32)
    chosen = sigma[inst_ids[:, None, None], source[None, None, :], local_pos[None, :, :]]
    physical = source[None, None, :] * slots + chosen
    owner_req = request_of[target[None, :, None] * rgroup + items // per_inst]
    block_ids = inst_ids[:, None, None] * per_inst + items % per_inst
    table = jnp.zeros((reqs, nblk), jnp.int32).at[owner_req.ravel(), block_ids.ravel()].set(physical.ravel())
    return (after, table)


def draw_place_after(key, part):
    return layout_plan(key)[0]


def draw_block_table(key, part):
    return layout_plan(key)[1]


def draw_queries(key, part):
    rows = N_INST // 2 * N_GROUP * PRE
    values = jax.random.normal(jax.random.fold_in(key, 21), (rows, HQ * HD), jnp.float32)
    return jnp.clip(values, -64.0, 64.0).astype(jnp.bfloat16)


def draw_old_cache(key, part):
    shape = (N_INST, N_GROUP * (N_INST // 2) * (CTX // BLK // N_INST), BLK, 2 * KVH * HD)
    values = jax.random.normal(jax.random.fold_in(key, 31), shape, jnp.float32)
    return jnp.clip(values, -64.0, 64.0).astype(jnp.bfloat16)


def set_ends(array, rng, smallest, high):
    spot = [jax.random.randint(jax.random.fold_in(rng, axis), (), 0, length) for axis, length in enumerate(array.shape)]
    widest = array.shape.index(max(array.shape))
    neighbour = spot[:widest] + [(spot[widest] + 1) % array.shape[widest]] + spot[widest + 1:]
    return array.at[tuple(spot)].set(smallest).at[tuple(neighbour)].set(high)


def block_scale(own_key, shape, shards, low, high):
    loudness = 1.0
    for axis_at, parts in shards:
        steps = jax.random.uniform(jax.random.fold_in(jax.random.fold_in(own_key, 6), axis_at), (parts,), jnp.float32, low / len(shards), high / len(shards))
        loudness = loudness * jnp.repeat(jnp.exp(steps), shape[axis_at] // parts).reshape((-1,) + (1,) * (len(shape) - 1 - axis_at))
    return loudness


def noise(stream_key, dims, spread, bound, cuts=(), kind=jnp.bfloat16):
    values = spread * jax.random.normal(stream_key, dims, jnp.float32)
    if cuts:
        values = values * block_scale(stream_key, dims, cuts, -0.22, 0.18)
    return jnp.clip(values, -bound, bound).astype(kind)


def setup_inputs(seed: int = 0) -> dict:
    seeds = jax.random.split(jax.random.key(seed), 7)
    old_cache = draw_old_cache(jax.random.fold_in(seeds[6], 71), 0)
    block_table = draw_block_table(jax.random.fold_in(seeds[6], 71), 0)
    place_after = draw_place_after(jax.random.fold_in(seeds[6], 71), 0)
    context_len = set_ends(jax.random.randint(seeds[3], (REQS,), CTX // 8, CTX + 1), jax.random.fold_in(seeds[3], 1), CTX // 8, CTX).astype(jnp.int32)
    queries = draw_queries(jax.random.fold_in(seeds[6], 71), 0)
    new_kv = noise(seeds[5], (REQS * PRE, 2 * KVH * HD), 1.0, 6.0, ((0, 256),))
    return {"old_cache": old_cache, "block_table": block_table, "place_after": place_after, "context_len": context_len, "queries": queries, "new_kv": new_kv}


def reference(old_cache, block_table, place_after, context_len, queries, new_kv):
    request_of = jnp.argsort(place_after).astype(jnp.int32)
    groups = HQ // KVH
    inst_of = (jnp.arange(NBLK, dtype=jnp.int32) // NBI).astype(jnp.int32)

    def one_slot(slot):
        request = request_of[slot]
        length = context_len[request]
        blocks = old_cache[inst_of, block_table[request]]
        cache = blocks.reshape(CTX, 2 * KVH * HD)
        fresh = lax.dynamic_slice_in_dim(new_kv, (slot * PRE).astype(jnp.int32), PRE, 0)
        asked = lax.dynamic_slice_in_dim(queries, (slot * PRE).astype(jnp.int32), PRE, 0)
        keyvals = jnp.concatenate([cache, fresh], axis=0).astype(jnp.float32)
        keys = keyvals[:, :KVH * HD].reshape(CTX + PRE, KVH, HD)
        values = keyvals[:, KVH * HD:].reshape(CTX + PRE, KVH, HD)
        heads = asked.astype(jnp.float32).reshape(PRE, KVH, groups, HD)
        scores = jnp.einsum("qhgd,khd->hgqk", heads, keys) * (HD ** -0.5)
        key_index = jnp.arange(CTX + PRE, dtype=jnp.int32)
        query_index = jnp.arange(PRE, dtype=jnp.int32)
        allowed = jnp.where(key_index[None, :] < CTX, key_index[None, :] < length,
                            key_index[None, :] - CTX <= query_index[:, None])
        scores = jnp.where(allowed[None, None], scores, -jnp.inf)
        largest = jnp.max(scores, axis=-1, keepdims=True)
        weights = jnp.exp(scores - largest).astype(jnp.bfloat16).astype(jnp.float32)
        total = jnp.sum(weights, axis=-1)
        summed = jnp.einsum("hgqk,khd->hgqd", weights, values)
        result = summed / total[..., None]
        return jnp.transpose(result, (2, 0, 1, 3)).reshape(PRE, HQ * HD).astype(jnp.bfloat16)

    outputs = lax.map(one_slot, jnp.arange(REQS, dtype=jnp.int32))
    return outputs.reshape(REQS * PRE, HQ * HD)
```

```python
import functools

import jax
import jax.numpy as jnp
from jax import lax
from jax.experimental import pallas as pl
from jax.experimental.pallas import tpu as pltpu
from jax.sharding import PartitionSpec as P

KVH = 8
HD = 128
NCH = 4
BIG = -1e30
MESH = pl.DeviceIdType.MESH


def tables(block_table, place_after, context_len, slots, per_inst):
    g = lax.axis_index("group")
    i = lax.axis_index("inst")
    ngroup = lax.axis_size("group")
    rgroup = slots // per_inst
    columns = lax.dynamic_slice_in_dim(block_table, i * per_inst, per_inst, 1)
    kk = lax.broadcasted_iota(jnp.int32, columns.shape, 1)
    keys = (place_after[:, None] * per_inst + kk).reshape(1, -1)
    places = columns.reshape(1, -1)
    ids = jnp.arange(slots, dtype=jnp.int32)
    mine = g * slots + ids
    key_of_slot = jnp.sum(jnp.where(places == mine[:, None], keys, 0), axis=1)
    rank = jnp.sum((key_of_slot[None, :] < key_of_slot[:, None]).astype(jnp.int32), axis=1)
    pos = (rank - g * (slots // ngroup) + slots) % slots
    send = jnp.sum(jnp.where(pos[None, :] == ids[:, None], ids[None, :], 0), axis=1)
    place_of_item = jnp.sum(jnp.where(keys == mine[:, None], places, 0), axis=1)
    owner = place_of_item // slots
    same = (owner[None, :] == owner[:, None]) & (ids[None, :] < ids[:, None])
    second = jnp.sum(same.astype(jnp.int32), axis=1)
    recv = ((g - owner + ngroup) % ngroup) * (slots // ngroup) + second
    slot = g * rgroup + i // 2
    length = jnp.sum(jnp.where(place_after == slot, context_len, 0))
    return jnp.concatenate([send, recv, jnp.broadcast_to(length, (slots,))])


def body(
    ngroup, ninst,
    tbl, cache, q, kv, out,
    cbuf, s1a, s1b, s1c, s1d, r1a, r1b, r1c, r1d, s2, r2,
    qx, kvx, qs, kbias, fbias, sref, mref, oo,
    ld, s1sem, r1sem, s2sem, r2sem, xs, xr, osem, orsem, lsem,
):
    g = lax.axis_index("group")
    i = lax.axis_index("inst")
    s1 = (s1a, s1b, s1c, s1d)
    r1 = (r1a, r1b, r1c, r1d)
    slots = cbuf.shape[0]
    tok = q.shape[0]
    half = lax.rem(i, 2)
    partner = i + 1 - 2 * half
    hw = q.shape[1] // 2
    kw = KVH * HD // 2

    loads = [
        pltpu.make_async_copy(cache.at[0], cbuf, ld.at[0]),
        pltpu.make_async_copy(q.at[:, pl.ds(half * hw, hw)], qx.at[0], ld.at[1]),
        pltpu.make_async_copy(kv.at[:, pl.ds(half * kw, kw)], kvx.at[0, 0], ld.at[2]),
        pltpu.make_async_copy(kv.at[:, pl.ds(2 * kw + half * kw, kw)], kvx.at[0, 1], ld.at[3]),
    ]
    for c in loads:
        c.start()

    barrier = pltpu.get_barrier_semaphore()

    def greet_group(d, _):
        pl.semaphore_signal(barrier, inc=1, device_id=(lax.rem(g + d, ngroup), i), device_id_type=MESH)
        return 0

    def greet_inst(e, _):
        pl.semaphore_signal(barrier, inc=1, device_id=(g, lax.rem(i + e, ninst)), device_id_type=MESH)
        return 0

    lax.fori_loop(1, ngroup, greet_group, 0)
    lax.fori_loop(1, ninst, greet_inst, 0)

    def tile_cols(c):
        return (c * HD, (KVH + c) * HD, (KVH // 2 + c) * HD, (KVH + KVH // 2 + c) * HD)

    def permute1(c):
        def step(p, _):
            s = tbl[p]
            for t, col in enumerate(tile_cols(c)):
                s1[c][p, t] = cbuf[s, :, col : col + HD]
            return 0

        lax.fori_loop(0, slots, step, 0, unroll=4)
        for p in range(slots // ngroup):
            r1[c][p] = s1[c][p]

    per = slots // ngroup

    def send1(c):
        def step(d, _):
            pltpu.make_async_remote_copy(
                src_ref=s1[c].at[pl.ds(per * d, per)],
                dst_ref=r1[c].at[pl.ds(per * d, per)],
                send_sem=s1sem.at[c],
                recv_sem=r1sem.at[c],
                device_id=(lax.rem(g + d, ngroup), i),
                device_id_type=MESH,
            ).start()
            return 0

        lax.fori_loop(1, ngroup, step, 0)

    def all1(c):
        return pltpu.make_async_remote_copy(
            src_ref=s1[c].at[pl.ds(per, slots - per)],
            dst_ref=r1[c].at[pl.ds(per, slots - per)],
            send_sem=s1sem.at[c],
            recv_sem=r1sem.at[c],
            device_id=(lax.rem(g + 1, ngroup), i),
            device_id_type=MESH,
        )

    items = slots // (ninst // 2)
    blk = cbuf.shape[1]

    def permute2(c):
        def gather(e, ref):
            j = lax.rem(i + e, ninst)
            w = j // 2
            h = lax.rem(j, 2)

            def step(k, _):
                idx = tbl[slots + w * items + k]
                for t in range(2):
                    ref[c, e, t, pl.ds(k * blk, blk), :] = r1[c][idx, 2 * h + t]
                return 0

            lax.fori_loop(0, items, step, 0, unroll=4)

        gather(0, r2)

        def outer(e, _):
            gather(e, s2)
            return 0

        lax.fori_loop(1, ninst, outer, 0)

    def send2(c):
        def step(e, _):
            pltpu.make_async_remote_copy(
                src_ref=s2.at[c, e],
                dst_ref=r2.at[c, e],
                send_sem=s2sem.at[c],
                recv_sem=r2sem.at[c],
                device_id=(g, lax.rem(i + e, ninst)),
                device_id_type=MESH,
            ).start()
            return 0

        lax.fori_loop(1, ninst, step, 0)

    def all2(c):
        return pltpu.make_async_remote_copy(
            src_ref=s2.at[c, pl.ds(1, ninst - 1)],
            dst_ref=r2.at[c, pl.ds(1, ninst - 1)],
            send_sem=s2sem.at[c],
            recv_sem=r2sem.at[c],
            device_id=(g, lax.rem(i + 1, ninst)),
            device_id_type=MESH,
        )

    other = 1 - half
    swaps = [
        pltpu.make_async_remote_copy(
            src_ref=src, dst_ref=dst, send_sem=xs.at[n], recv_sem=xr.at[n],
            device_id=(g, partner), device_id_type=MESH,
        )
        for n, (src, dst) in enumerate([
            (q.at[:, pl.ds(other * hw, hw)], qx.at[1]),
            (kv.at[:, pl.ds(other * kw, kw)], kvx.at[1, 0]),
            (kv.at[:, pl.ds(2 * kw + other * kw, kw)], kvx.at[1, 1]),
        ])
    ]

    loads[0].wait()
    permute1(0)
    pl.semaphore_wait(barrier, ngroup - 1 + ninst - 1)
    send1(0)
    for copy in swaps:
        copy.start()
    for c in range(1, NCH):
        permute1(c)
        send1(c)

    length = tbl[2 * slots]
    ctx = items * blk
    eye = (
        lax.broadcasted_iota(jnp.int32, (tok, tok), 0)
        == lax.broadcasted_iota(jnp.int32, (tok, tok), 1)
    )
    for b in range(qs.shape[0] // tok):
        qs[pl.ds(b * tok, tok), HD:] = jnp.where(eye, 1.0, 0.0).astype(jnp.bfloat16)
    row = lax.broadcasted_iota(jnp.int32, (ctx, HD), 0)
    for e in range(ninst):
        source = lax.rem(i - e + ninst, ninst)
        kbias[e] = jnp.where(row + source * ctx < length, 0.0, BIG).astype(jnp.bfloat16)
    key = lax.broadcasted_iota(jnp.int32, (tok, HD), 0)
    query = lax.broadcasted_iota(jnp.int32, (tok, HD), 1)
    tri = jnp.where(key <= query, 0.0, BIG).astype(jnp.bfloat16)
    flag = jnp.full((tok, HD), half, jnp.int32)
    fbias[0, :tok, :] = tri
    fbias[0, tok:, :] = jnp.where(flag == 1, 0.0, BIG).astype(jnp.bfloat16)
    fbias[1, :tok, :] = jnp.where(flag == 0, 0.0, BIG).astype(jnp.bfloat16)
    fbias[1, tok:, :] = tri

    for c in range(NCH):
        all1(c).wait_recv()
        permute2(c)
        send2(c)

    for copy in loads[1:]:
        copy.wait()
    for copy in swaps:
        copy.wait_recv()

    groups = hw // (KVH // 2 * HD)
    rows = groups * tok
    coef = float(HD) ** -0.5 * 1.4426950408889634
    nt = (((1,), (1,)), ((), ()))

    def score(qv, k, bias):
        return lax.dot_general(
            qv, jnp.concatenate([k, bias], axis=1), nt, preferred_element_type=jnp.float32
        )

    def attention(c):
        for h in range(2):
            for j in range(groups):
                qs[pl.ds((h * groups + j) * tok, tok), :HD] = qx[h, :, pl.ds((groups * c + j) * HD, HD)]
        kf = jnp.concatenate([kvx[0, 0, :, pl.ds(c * HD, HD)], kvx[1, 0, :, pl.ds(c * HD, HD)]], axis=0)
        vf = jnp.concatenate([kvx[0, 1, :, pl.ds(c * HD, HD)], kvx[1, 1, :, pl.ds(c * HD, HD)]], axis=0)
        for h in range(2):
            s = score(qs[pl.ds(h * rows, rows), :], kf, fbias[h])
            sref[ninst, pl.ds(h * rows, rows), :] = s
            mref[pl.ds(h * rows, rows), :] = jnp.maximum(s[:, :HD], s[:, HD:])

        def first(e, _):
            s = score(qs[...], r2[c, e, 0], kbias[e])
            sref[e] = s
            mref[...] = jnp.maximum(mref[...], jnp.maximum(s[:, :HD], s[:, HD:]))
            return 0

        lax.fori_loop(0, ninst, first, 0)
        rb = 2 * tok
        ones = jnp.ones((ctx, HD), jnp.bfloat16)

        def second(b, _):
            span = pl.ds(pl.multiple_of(b * rb, rb), rb)
            m = jnp.max(mref[span, :], axis=1, keepdims=True)
            total = jnp.zeros((rb, 2 * HD), jnp.float32)
            for e in range(ninst + 1):
                p = jnp.exp2((sref[e, span, :] - m) * coef).astype(jnp.bfloat16)
                v = r2[c, e, 1] if e < ninst else vf
                total = total + jnp.dot(
                    p, jnp.concatenate([v, ones], axis=1), preferred_element_type=jnp.float32
                )
            o = (total[:, :HD] / total[:, HD:]).astype(jnp.bfloat16)
            oo[c, 2 * b] = o[:tok]
            oo[c, 2 * b + 1] = o[tok:]
            return 0

        lax.fori_loop(0, qs.shape[0] // rb, second, 0)

    pending = []
    for c in range(NCH):
        all2(c).wait_recv()
        attention(c)
        for j in range(groups):
            col = half * hw + (c * groups + j) * HD
            mine = pltpu.make_async_copy(oo.at[c, j], out.at[:, pl.ds(col, HD)], lsem.at[c, j])
            mine.start()
            theirs = pltpu.make_async_remote_copy(
                src_ref=oo.at[c, groups + j],
                dst_ref=out.at[:, pl.ds(col, HD)],
                send_sem=osem.at[c, j],
                recv_sem=orsem.at[c, j],
                device_id=(g, partner),
                device_id_type=MESH,
            )
            theirs.start()
            pending.append((mine, theirs))
    for copy in swaps:
        copy.wait_send()
    for c in range(NCH):
        all1(c).wait_send()
        all2(c).wait_send()
    for mine, theirs in pending:
        mine.wait()
        theirs.wait()


def on_device(old_cache, block_table, place_after, context_len, queries, new_kv):
    ninst = lax.axis_size("inst")
    ngroup = lax.axis_size("group")
    slots, blk, width = old_cache.shape[1:]
    tok, qw = queries.shape
    per_inst = block_table.shape[1] // ninst
    tbl = tables(block_table, place_after, context_len, slots, per_inst)
    ctx = per_inst * blk
    groups = qw // (KVH * HD)
    bf = jnp.bfloat16
    piece = pltpu.VMEM((slots, 4, blk, HD), bf)
    rows = 2 * groups * tok
    dma = pltpu.SemaphoreType.DMA
    return pl.pallas_call(
        functools.partial(body, ngroup, ninst),
        out_shape=jax.ShapeDtypeStruct((tok, qw), bf),
        in_specs=[pl.BlockSpec(memory_space=pltpu.SMEM)] + [pl.BlockSpec(memory_space=pl.ANY)] * 3,
        out_specs=pl.BlockSpec(memory_space=pl.ANY),
        scratch_shapes=[
            pltpu.VMEM((slots, blk, width), bf),
            *[piece] * (2 * NCH),
            pltpu.VMEM((NCH, ninst, 2, ctx, HD), bf),
            pltpu.VMEM((NCH, ninst, 2, ctx, HD), bf),
            pltpu.VMEM((2, tok, qw // 2), bf),
            pltpu.VMEM((2, 2, tok, KVH // 2 * HD), bf),
            pltpu.VMEM((rows, 2 * HD), bf),
            pltpu.VMEM((ninst, ctx, HD), bf),
            pltpu.VMEM((2, 2 * tok, HD), bf),
            pltpu.VMEM((ninst + 1, rows, ctx), jnp.float32),
            pltpu.VMEM((rows, HD), jnp.float32),
            pltpu.VMEM((NCH, 2 * groups, tok, HD), bf),
            dma((4,)), dma((NCH,)), dma((NCH,)), dma((NCH,)), dma((NCH,)),
            dma((3,)), dma((3,)), dma((NCH, groups)), dma((NCH, groups)), dma((NCH, groups)),
        ],
        compiler_params=pltpu.CompilerParams(
            collective_id=0, has_side_effects=True, vmem_limit_bytes=60 * 1024 * 1024
        ),
    )(tbl, old_cache, queries, new_kv)


def solution(mesh):
    return jax.shard_map(
        on_device,
        mesh=mesh,
        in_specs=(
            P("inst", "group", None, None),
            P(),
            P(),
            P(),
            P(("group", "inst"), None),
            P(("group", "inst"), None),
        ),
        out_specs=P(("group", "inst"), None),
        check_vma=False,
    )
```

```python
import functools

import jax
import jax.numpy as jnp
from jax import lax
from jax.experimental import pallas as pl
from jax.experimental.pallas import tpu as pltpu
from jax.sharding import PartitionSpec as P

KVH = 8
HD = 128
NCH = KVH
LAG = 3
BIG = -1e30
COEF = float(HD) ** -0.5 * 1.4426950408889634
MESH = pl.DeviceIdType.MESH


def tables(block_table, place_after, context_len, slots, per_inst):
    g = lax.axis_index("group")
    i = lax.axis_index("inst")
    ngroup = lax.axis_size("group")
    rgroup = slots // per_inst
    columns = lax.dynamic_slice_in_dim(block_table, i * per_inst, per_inst, 1)
    kk = lax.broadcasted_iota(jnp.int32, columns.shape, 1)
    keys = (place_after[:, None] * per_inst + kk).reshape(1, -1)
    places = columns.reshape(1, -1)
    ids = jnp.arange(slots, dtype=jnp.int32)
    mine = g * slots + ids
    key_of_slot = jnp.sum(jnp.where(places == mine[:, None], keys, 0), axis=1)
    rank = jnp.sum((key_of_slot[None, :] < key_of_slot[:, None]).astype(jnp.int32), axis=1)
    pos = (rank - g * (slots // ngroup) + slots) % slots
    send = jnp.sum(jnp.where(pos[None, :] == ids[:, None], ids[None, :], 0), axis=1)
    place_of_item = jnp.sum(jnp.where(keys == mine[:, None], places, 0), axis=1)
    owner = place_of_item // slots
    same = (owner[None, :] == owner[:, None]) & (ids[None, :] < ids[:, None])
    second = jnp.sum(same.astype(jnp.int32), axis=1)
    recv = ((g - owner + ngroup) % ngroup) * (slots // ngroup) + second
    slot = g * rgroup + i // 2
    length = jnp.sum(jnp.where(place_after == slot, context_len, 0))
    return jnp.concatenate([send, recv, jnp.broadcast_to(length, (slots,))])


def body(ngroup, ninst, tbl, cache, q, kv, out, *scratch):
    s1, r1 = scratch[:NCH], scratch[NCH : 2 * NCH]
    (cbuf, s2, r2, qx, kvx, qs, kbias, fbias, sref, sfresh, mref, own, stat, oo, orecv, st, strecv,
     ostage, ld, s1sem, r1sem, s2sem, r2sem, xs, xr, osem, orsem, tsem, trsem, lsem) = scratch[2 * NCH :]
    g = lax.axis_index("group")
    i = lax.axis_index("inst")
    slots, blk = cbuf.shape[:2]
    tok = q.shape[0]
    half = lax.rem(i, 2)
    sgn = 1 - 2 * half
    partner = i + sgn
    kw = KVH * HD
    groups = q.shape[1] // kw
    rows = groups * tok
    per = slots // ngroup
    items = slots // (ninst // 2)
    ctx = items * blk
    sides = ninst // 2

    loads = [
        pltpu.make_async_copy(cache.at[0], cbuf, ld.at[0]),
        pltpu.make_async_copy(q, qx.at[0], ld.at[1]),
        pltpu.make_async_copy(kv, kvx, ld.at[2]),
    ]
    for copy in loads:
        copy.start()

    barrier = pltpu.get_barrier_semaphore()

    def greet_group(d, _):
        pl.semaphore_signal(barrier, inc=1, device_id=(lax.rem(g + d, ngroup), i), device_id_type=MESH)
        return 0

    def greet_inst(e, _):
        pl.semaphore_signal(barrier, inc=1, device_id=(g, lax.rem(i + e, ninst)), device_id_type=MESH)
        return 0

    lax.fori_loop(1, ngroup, greet_group, 0)
    lax.fori_loop(1, ninst, greet_inst, 0)

    def permute1(c):
        def step(p, _):
            s = tbl[p]
            s1[c][p, 0] = cbuf[s, :, c * HD : (c + 1) * HD]
            s1[c][p, 1] = cbuf[s, :, kw + c * HD : kw + (c + 1) * HD]
            return 0

        lax.fori_loop(0, slots, step, 0, unroll=8)
        for p in range(per):
            r1[c][p] = s1[c][p]

    def send1(c):
        def step(d, _):
            pltpu.make_async_remote_copy(
                src_ref=s1[c].at[pl.ds(per * d, per)],
                dst_ref=r1[c].at[pl.ds(per * d, per)],
                send_sem=s1sem.at[c],
                recv_sem=r1sem.at[c],
                device_id=(lax.rem(g + d, ngroup), i),
                device_id_type=MESH,
            ).start()
            return 0

        lax.fori_loop(1, ngroup, step, 0)

    def all1(c):
        return pltpu.make_async_remote_copy(
            src_ref=s1[c].at[pl.ds(per, slots - per)],
            dst_ref=r1[c].at[pl.ds(per, slots - per)],
            send_sem=s1sem.at[c],
            recv_sem=r1sem.at[c],
            device_id=(lax.rem(g + 1, ngroup), i),
            device_id_type=MESH,
        )

    def target(n):
        step = (0, -1, 2, -3)[n]
        return lax.rem(i + sgn * step + ninst, ninst)

    def permute2(c):
        for n in range(sides):
            base = slots + target(n) // 2 * items

            def step(k, _):
                idx = tbl[base + k]
                for t in range(2):
                    if n == 0:
                        r2[c, 0, t, pl.ds(k * blk, blk), :] = r1[c][idx, t]
                    else:
                        s2[c, n - 1, t, pl.ds(k * blk, blk), :] = r1[c][idx, t]
                return 0

            lax.fori_loop(0, items, step, 0, unroll=8)

    def send2(c):
        for n in range(sides - 1, 0, -1):
            pltpu.make_async_remote_copy(
                src_ref=s2.at[c, n - 1],
                dst_ref=r2.at[c, n],
                send_sem=s2sem.at[c],
                recv_sem=r2sem.at[c],
                device_id=(g, target(n)),
                device_id_type=MESH,
            ).start()

    def all2(c):
        return pltpu.make_async_remote_copy(
            src_ref=s2.at[c],
            dst_ref=r2.at[c, pl.ds(1, sides - 1)],
            send_sem=s2sem.at[c],
            recv_sem=r2sem.at[c],
            device_id=(g, partner),
            device_id_type=MESH,
        )

    def to_partner(src, dst, ssem, rsem):
        return pltpu.make_async_remote_copy(
            src_ref=src, dst_ref=dst, send_sem=ssem, recv_sem=rsem,
            device_id=(g, partner), device_id_type=MESH,
        )

    swap = to_partner(q, qx.at[1], xs, xr)

    loads[0].wait()
    permute1(0)
    pl.semaphore_wait(barrier, ngroup - 1 + ninst - 1)
    send1(0)
    swap.start()
    for c in range(1, NCH):
        permute1(c)
        send1(c)

    length = tbl[2 * slots]
    eye = (
        lax.broadcasted_iota(jnp.int32, (tok, tok), 0)
        == lax.broadcasted_iota(jnp.int32, (tok, tok), 1)
    )
    for b in range(groups):
        qs[pl.ds(b * tok, tok), HD:] = jnp.where(eye, 1.0, 0.0).astype(jnp.bfloat16)
    row = lax.broadcasted_iota(jnp.int32, (ctx, HD), 0)
    for n in range(sides):
        source = lax.rem(i - sgn * n + ninst, ninst)
        kbias[n] = jnp.where(row + source * ctx < length, 0.0, BIG).astype(jnp.bfloat16)
    key = lax.broadcasted_iota(jnp.int32, (tok, HD), 0)
    query = lax.broadcasted_iota(jnp.int32, (tok, HD), 1)
    fbias[0] = jnp.where(key <= query, 0.0, BIG).astype(jnp.bfloat16)
    flag = jnp.full((tok, HD), half, jnp.int32)
    fbias[1] = jnp.where(flag == 0, 0.0, BIG).astype(jnp.bfloat16)

    nt = (((1,), (1,)), ((), ()))

    def score(k, bias):
        return lax.dot_general(
            qs[...], jnp.concatenate([k, bias], axis=1), nt, preferred_element_type=jnp.float32
        )

    lane = lax.broadcasted_iota(jnp.int32, (tok, HD), 1)
    rb = 2 * tok
    ones = jnp.ones((ctx, HD), jnp.bfloat16)

    def attend(c, h):
        for j in range(groups):
            qs[pl.ds(j * tok, tok), :HD] = qx[h, :, (groups * c + j) * HD : (groups * c + j + 1) * HD]
        s = score(kvx[:, c * HD : (c + 1) * HD], fbias[h])
        sfresh[...] = s
        mref[...] = s

        def first(n, _):
            s = score(r2[c, n, 0], kbias[n])
            sref[n] = s
            mref[...] = jnp.maximum(mref[...], jnp.maximum(s[:, :HD], s[:, HD:]))
            return 0

        lax.fori_loop(0, sides, first, 0)
        vf = kvx[:, kw + c * HD : kw + (c + 1) * HD]
        stats = jnp.zeros((tok, HD), jnp.float32)
        for b in range(rows // rb):
            span = pl.ds(b * rb, rb)
            m = jnp.max(mref[span, :], axis=1, keepdims=True)
            total = jnp.dot(
                jnp.exp2((sfresh[span, :] - m) * COEF).astype(jnp.bfloat16),
                jnp.concatenate([vf, ones[:tok]], axis=1),
                preferred_element_type=jnp.float32,
            )
            for n in range(sides):
                p = jnp.exp2((sref[n, span, :] - m) * COEF).astype(jnp.bfloat16)
                total = total + jnp.dot(
                    p, jnp.concatenate([r2[c, n, 1], ones], axis=1), preferred_element_type=jnp.float32
                )
            o = total[:, :HD] / total[:, HD:]
            for j in range(rb // tok):
                at = b * (rb // tok) + j
                part = slice(j * tok, (j + 1) * tok)
                stats = jnp.where(lane == at, m[part], stats)
                stats = jnp.where(lane == groups + at, total[part, HD:], stats)
                if h == 0:
                    own[c % 2, at] = o[part]
                else:
                    oo[c, at] = o[part].astype(jnp.bfloat16)
        if h == 0:
            stat[c % 2] = stats
        else:
            st[c] = jnp.transpose(stats)[: 2 * groups]

    def combine(c):
        oparts[c].wait_recv()
        tparts[c].wait_recv()
        fill = jnp.zeros((tok - 2 * groups, HD), jnp.float32)
        theirs = jnp.transpose(jnp.concatenate([strecv[c], fill], axis=0))
        mine = stat[c % 2]
        top = jnp.maximum(mine, theirs)
        for j in range(groups):
            a, b = slice(j, j + 1), slice(groups + j, groups + j + 1)
            wa = mine[:, b] * jnp.exp2((mine[:, a] - top[:, a]) * COEF)
            wb = theirs[:, b] * jnp.exp2((theirs[:, a] - top[:, a]) * COEF)
            r = 1.0 / (wa + wb)
            o = own[c % 2, j] * (wa * r) + orecv[c, j].astype(jnp.float32) * (wb * r)
            ostage[c, :, j * HD : (j + 1) * HD] = o.astype(jnp.bfloat16)
        outs[c].start()

    oparts = [to_partner(oo.at[c], orecv.at[c], osem.at[c], orsem.at[c]) for c in range(NCH)]
    tparts = [to_partner(st.at[c], strecv.at[c], tsem.at[c], trsem.at[c]) for c in range(NCH)]
    outs = [
        pltpu.make_async_copy(
            ostage.at[c], out.at[:, pl.ds(c * groups * HD, groups * HD)], lsem.at[c]
        )
        for c in range(NCH)
    ]

    def attention(c):
        if c == 0:
            for copy in loads[1:]:
                copy.wait()
            swap.wait_recv()
        all2(c).wait_recv()
        attend(c, 1)
        tparts[c].start()
        oparts[c].start()
        attend(c, 0)
        if c:
            combine(c - 1)

    for c in range(NCH):
        all1(c).wait_recv()
        permute2(c)
        send2(c)
        if c >= LAG:
            attention(c - LAG)
    for c in range(NCH - LAG, NCH):
        attention(c)
    combine(NCH - 1)
    swap.wait_send()
    for c in range(NCH):
        all1(c).wait_send()
        all2(c).wait_send()
        oparts[c].wait_send()
        tparts[c].wait_send()
        outs[c].wait()


def on_device(old_cache, block_table, place_after, context_len, queries, new_kv):
    ninst = lax.axis_size("inst")
    ngroup = lax.axis_size("group")
    slots, blk, width = old_cache.shape[1:]
    tok, qw = queries.shape
    per_inst = block_table.shape[1] // ninst
    tbl = tables(block_table, place_after, context_len, slots, per_inst)
    ctx = per_inst * blk
    groups = qw // (KVH * HD)
    rows = groups * tok
    sides = ninst // 2
    bf, f32 = jnp.bfloat16, jnp.float32
    dma = pltpu.SemaphoreType.DMA
    return pl.pallas_call(
        functools.partial(body, ngroup, ninst),
        out_shape=jax.ShapeDtypeStruct((tok, qw), bf),
        in_specs=[pl.BlockSpec(memory_space=pltpu.SMEM)] + [pl.BlockSpec(memory_space=pl.ANY)] * 3,
        out_specs=pl.BlockSpec(memory_space=pl.ANY),
        scratch_shapes=[
            *[pltpu.VMEM((slots, 2, blk, HD), bf)] * (2 * NCH),
            pltpu.VMEM((slots, blk, width), bf),
            pltpu.VMEM((NCH, sides - 1, 2, ctx, HD), bf),
            pltpu.VMEM((NCH, sides, 2, ctx, HD), bf),
            pltpu.VMEM((2, tok, qw), bf),
            pltpu.VMEM((tok, 2 * KVH * HD), bf),
            pltpu.VMEM((rows, 2 * HD), bf),
            pltpu.VMEM((sides, ctx, HD), bf),
            pltpu.VMEM((2, tok, HD), bf),
            pltpu.VMEM((sides, rows, ctx), f32),
            pltpu.VMEM((rows, tok), f32),
            pltpu.VMEM((rows, HD), f32),
            pltpu.VMEM((2, groups, tok, HD), f32),
            pltpu.VMEM((2, tok, HD), f32),
            pltpu.VMEM((NCH, groups, tok, HD), bf),
            pltpu.VMEM((NCH, groups, tok, HD), bf),
            pltpu.VMEM((NCH, 2 * groups, HD), f32),
            pltpu.VMEM((NCH, 2 * groups, HD), f32),
            pltpu.VMEM((NCH, tok, groups * HD), bf),
            dma((3,)), dma((NCH,)), dma((NCH,)), dma((NCH,)), dma((NCH,)), dma, dma,
            dma((NCH,)), dma((NCH,)), dma((NCH,)), dma((NCH,)), dma((NCH,)),
        ],
        compiler_params=pltpu.CompilerParams(
            collective_id=0, has_side_effects=True, vmem_limit_bytes=60 * 1024 * 1024
        ),
    )(tbl, old_cache, queries, new_kv)


def solution(mesh):
    return jax.shard_map(
        on_device,
        mesh=mesh,
        in_specs=(
            P("inst", "group", None, None),
            P(),
            P(),
            P(),
            P(("group", "inst"), None),
            P(("group", "inst"), None),
        ),
        out_specs=P(("group", "inst"), None),
        check_vma=False,
    )
```

```python
import functools

import jax
import jax.numpy as jnp
from jax import lax
from jax.experimental import pallas as pl
from jax.experimental.pallas import tpu as pltpu
from jax.sharding import PartitionSpec as P

KVH = 8
HD = 128
PARTS = [(0, (0,)), (0, (1,))] + [(c, (0, 1)) for c in range(1, KVH)]
EARLY = 4
VLIM = 46
BIG = -1e30
COEF = float(HD) ** -0.5 * 1.4426950408889634
MESH = pl.DeviceIdType.MESH


def onehot(cond):
    return jnp.where(cond, 1.0, 0.0).astype(jnp.bfloat16)


def tables(blocks, places, tab, g, i, ngroup, slots, items):
    reqs, nblk = blocks.shape
    rgroup = slots // items
    value = blocks[...]
    owner = (value // slots).astype(jnp.float32).astype(jnp.bfloat16)
    local = (value % slots).astype(jnp.float32).astype(jnp.bfloat16)
    k = lax.broadcasted_iota(jnp.int32, (nblk, HD), 0)
    lane = lax.broadcasted_iota(jnp.int32, (nblk, HD), 1)
    pick = onehot(k == i * items + lane % items)
    row = lax.broadcasted_iota(jnp.int32, (rgroup * ngroup, reqs), 0)
    place = row % ngroup * rgroup + row // ngroup
    order = onehot(jnp.broadcast_to(places[...], (rgroup * ngroup, reqs)) == place)

    def by_group(array):
        columns = jnp.dot(array, pick, preferred_element_type=jnp.float32).astype(jnp.bfloat16)
        rows = jnp.dot(order, columns, preferred_element_type=jnp.float32)
        within = lax.broadcasted_iota(jnp.int32, (ngroup, HD), 1) // items
        result = rows[:ngroup]
        for w in range(1, rgroup):
            result = jnp.where(within == w, rows[w * ngroup : (w + 1) * ngroup], result)
        return result.astype(jnp.int32)

    owners, locals_ = by_group(owner), by_group(local)
    item = lax.broadcasted_iota(jnp.int32, (ngroup, HD), 1)
    hit = (owners == g) & (item < slots)
    first = jnp.min(jnp.where(hit, item, HD), axis=1, keepdims=True)
    last = jnp.max(jnp.where(hit, item, -1), axis=1, keepdims=True)
    one = jnp.sum(jnp.where(item == first, locals_, 0), axis=1, keepdims=True)
    two = jnp.sum(jnp.where(item == last, locals_, 0), axis=1, keepdims=True)
    tab[:ngroup, :] = jnp.where(item == 0, one, two)
    mine = jnp.sum(
        jnp.where(lax.broadcasted_iota(jnp.int32, (ngroup, HD), 0) == g, owners, 0), axis=0, keepdims=True
    )
    across = jnp.broadcast_to(mine, (HD, HD)).astype(jnp.float32)
    down = jnp.transpose(across)
    t0 = lax.broadcasted_iota(jnp.int32, (HD, HD), 0)
    t1 = lax.broadcasted_iota(jnp.int32, (HD, HD), 1)
    before = jnp.sum(jnp.where((across == down) & (t0 < t1), 1, 0), axis=0, keepdims=True)
    per = slots // ngroup
    arrival = (g - mine + ngroup) % ngroup * per + jnp.minimum(before, per - 1)
    tab[ngroup:, :] = jnp.broadcast_to(arrival, (tab.shape[0] - ngroup, HD))


def body(ngroup, ninst, blocks_hbm, places_hbm, lengths_hbm, cache_hbm, q, kv, out, *scratch):
    parts = len(PARTS)
    s1, r1 = scratch[:parts], scratch[parts : 2 * parts]
    (cache, blocks, places, lengths, tab, tbl, s2, r2, qx, kvx, qs, kbias, fbias, sref, sfresh, mref, own, stat, oo, orecv, st, strecv,
     ld, s1sem, r1sem, s2sem, r2sem, xs, xr, osem, orsem, tsem, trsem) = scratch[2 * parts :]
    g = lax.axis_index("group")
    i = lax.axis_index("inst")
    slots, blk = cache.shape[:2]
    tok = q.shape[0]
    half = lax.rem(i, 2)
    sgn = 1 - 2 * half
    partner = i + sgn
    kw = KVH * HD
    groups = q.shape[1] // kw
    qw = groups * HD
    rows = groups * tok
    per = slots // ngroup
    items = slots // (ninst // 2)
    ctx = items * blk
    sides = ninst // 2

    pairs = [
        (blocks_hbm, blocks), (places_hbm, places), (lengths_hbm, lengths),
        (cache_hbm.at[0], cache), (kv, kvx), (q, qx.at[1]),
    ]
    loads = [pltpu.make_async_copy(src, dst, ld.at[n]) for n, (src, dst) in enumerate(pairs)]
    for copy in loads:
        copy.start()

    barrier = pltpu.get_barrier_semaphore()

    def greet_group(d, _):
        pl.semaphore_signal(barrier, inc=1, device_id=(lax.rem(g + d, ngroup), i), device_id_type=MESH)
        return 0

    def greet_inst(e, _):
        pl.semaphore_signal(barrier, inc=1, device_id=(g, lax.rem(i + e, ninst)), device_id_type=MESH)
        return 0

    lax.fori_loop(1, ngroup, greet_group, 0)
    lax.fori_loop(1, ninst, greet_inst, 0)


    def permute1(p):
        c, kinds = PARTS[p]

        def step(k, _):
            s = tbl[lax.rem(g + k // per, ngroup), lax.rem(k, per)]
            for n, t in enumerate(kinds):
                s1[p][k, n] = cache[s, :, t * kw + c * HD : t * kw + (c + 1) * HD]
            return 0

        lax.fori_loop(0, slots, step, 0, unroll=8)
        for k in range(per):
            r1[p][k] = s1[p][k]

    def send1(p):
        def step(d, _):
            pltpu.make_async_remote_copy(
                src_ref=s1[p].at[pl.ds(per * d, per)],
                dst_ref=r1[p].at[pl.ds(per * d, per)],
                send_sem=s1sem.at[p],
                recv_sem=r1sem.at[p],
                device_id=(lax.rem(g + d, ngroup), i),
                device_id_type=MESH,
            ).start()
            return 0

        lax.fori_loop(1, ngroup, step, 0)

    def all1(p):
        return pltpu.make_async_remote_copy(
            src_ref=s1[p].at[pl.ds(per, slots - per)],
            dst_ref=r1[p].at[pl.ds(per, slots - per)],
            send_sem=s1sem.at[p],
            recv_sem=r1sem.at[p],
            device_id=(lax.rem(g + 1, ngroup), i),
            device_id_type=MESH,
        )

    def target(n):
        step = (0, -1, 2, -3)[n]
        return lax.rem(i + sgn * step + ninst, ninst)

    def permute2(p):
        c, kinds = PARTS[p]
        for n in range(sides):
            base = target(n) // 2 * items

            def step(k, _):
                idx = tbl[ngroup, base + k]
                for m, t in enumerate(kinds):
                    if n == 0:
                        r2[c, t, 0, pl.ds(k * blk, blk), :] = r1[p][idx, m]
                    else:
                        s2[c, t, n - 1, pl.ds(k * blk, blk), :] = r1[p][idx, m]
                return 0

            lax.fori_loop(0, items, step, 0, unroll=8)

    def send2(c, t):
        for n in range(sides - 1, 0, -1):
            pltpu.make_async_remote_copy(
                src_ref=s2.at[c, t, n - 1],
                dst_ref=r2.at[c, t, n],
                send_sem=s2sem.at[c, t],
                recv_sem=r2sem.at[c, t],
                device_id=(g, target(n)),
                device_id_type=MESH,
            ).start()

    def all2(c, t):
        return pltpu.make_async_remote_copy(
            src_ref=s2.at[c, t],
            dst_ref=r2.at[c, t, pl.ds(1, sides - 1)],
            send_sem=s2sem.at[c, t],
            recv_sem=r2sem.at[c, t],
            device_id=(g, partner),
            device_id_type=MESH,
        )

    def to_partner(src, dst, ssem, rsem):
        return pltpu.make_async_remote_copy(
            src_ref=src, dst_ref=dst, send_sem=ssem, recv_sem=rsem,
            device_id=(g, partner), device_id_type=MESH,
        )

    def swap(c):
        cols = pl.ds(pl.multiple_of(c * qw, qw), qw)
        return to_partner(q.at[:, cols], qx.at[0, :, cols], xs.at[c], xr.at[c])

    for copy in loads[:3]:
        copy.wait()
    tables(blocks, places, tab, g, i, ngroup, slots, items)
    to_scalars = pltpu.make_async_copy(tab, tbl, ld.at[len(pairs)])
    to_scalars.start()
    loads[3].wait()
    to_scalars.wait()
    permute1(0)
    pl.semaphore_wait(barrier, ngroup - 1 + ninst - 1)
    send1(0)
    permute1(1)
    send1(1)
    for c in range(EARLY):
        swap(c).start()
    for p in range(2, parts):
        permute1(p)
        send1(p)

    slot = g * (slots // items) + i // 2
    length = jnp.sum(jnp.where(places[...] == slot, lengths[...], 0), axis=1, keepdims=True)
    eye = (
        lax.broadcasted_iota(jnp.int32, (tok, tok), 0)
        == lax.broadcasted_iota(jnp.int32, (tok, tok), 1)
    )
    for b in range(2 * groups):
        qs[pl.ds(b * tok, tok), HD:] = jnp.where(eye, 1.0, 0.0).astype(jnp.bfloat16)
    row = lax.broadcasted_iota(jnp.int32, (ctx, HD), 0)
    for n in range(sides):
        source = lax.rem(i - sgn * n + ninst, ninst)
        kbias[n] = jnp.where(row + source * ctx < length, 0.0, BIG).astype(jnp.bfloat16)
    key = lax.broadcasted_iota(jnp.int32, (tok, HD), 0)
    query = lax.broadcasted_iota(jnp.int32, (tok, HD), 1)
    flag = jnp.full((tok, HD), half, jnp.int32)
    fbias[0] = jnp.where(flag == 0, 0.0, BIG).astype(jnp.bfloat16)
    fbias[1] = jnp.where(key <= query, 0.0, BIG).astype(jnp.bfloat16)

    for p, (c, kinds) in enumerate(PARTS):
        all1(p).wait_recv()
        permute2(p)
        for t in kinds:
            send2(c, t)
        if 1 in kinds and c + EARLY < KVH:
            swap(c + EARLY).start()

    for copy in loads[4:]:
        copy.wait()

    nt = (((1,), (1,)), ((), ()))

    def score(qv, k, bias):
        return lax.dot_general(
            qv, jnp.concatenate([k, bias], axis=1), nt, preferred_element_type=jnp.float32
        )

    lane = lax.broadcasted_iota(jnp.int32, (tok, HD), 1)
    rb = 2 * tok
    ones = jnp.ones((ctx, HD), jnp.bfloat16)

    def scores(c):
        for h in range(2):
            for j in range(groups):
                qs[pl.ds((h * groups + j) * tok, tok), :HD] = qx[
                    h, :, pl.ds(pl.multiple_of(c * qw + j * HD, HD), HD)
                ]
            span = pl.ds(h * rows, rows)
            s = score(qs[span, :], kvx[:, pl.ds(pl.multiple_of(c * HD, HD), HD)], fbias[h])
            sfresh[span, :] = s
            mref[span, :] = s

        def first(n, _):
            s = score(qs[...], r2[c, 0, n], kbias[n])
            sref[n] = s
            mref[...] = jnp.maximum(mref[...], jnp.maximum(s[:, :HD], s[:, HD:]))
            return 0

        lax.fori_loop(0, sides, first, 0)

    def values(c, h):
        vf = kvx[:, pl.ds(pl.multiple_of(kw + c * HD, HD), HD)]
        stats = jnp.zeros((tok, HD), jnp.float32)
        for b in range(rows // rb):
            span = pl.ds(h * rows + b * rb, rb)
            m = jnp.max(mref[span, :], axis=1, keepdims=True)
            total = jnp.dot(
                jnp.exp2((sfresh[span, :] - m) * COEF).astype(jnp.bfloat16),
                jnp.concatenate([vf, ones[:tok]], axis=1),
                preferred_element_type=jnp.float32,
            )
            for n in range(sides):
                w = jnp.exp2((sref[n, span, :] - m) * COEF).astype(jnp.bfloat16)
                total = total + jnp.dot(
                    w, jnp.concatenate([r2[c, 1, n], ones], axis=1), preferred_element_type=jnp.float32
                )
            o = total[:, :HD] / total[:, HD:]
            for j in range(rb // tok):
                at = b * (rb // tok) + j
                part = slice(j * tok, (j + 1) * tok)
                stats = jnp.where(lane == at, m[part], stats)
                stats = jnp.where(lane == groups + at, total[part, HD:], stats)
                if h == 1:
                    own[lax.rem(c, 2), at] = o[part]
                else:
                    oo[c, at] = o[part].astype(jnp.bfloat16)
        if h == 1:
            stat[lax.rem(c, 2)] = stats
        else:
            st[c] = jnp.transpose(stats)[: 2 * groups]

    def opart(c):
        return to_partner(oo.at[c], orecv.at[c], osem.at[c], orsem.at[c])

    def tpart(c):
        return to_partner(st.at[c], strecv.at[c], tsem.at[c], trsem.at[c])

    def combine(c):
        opart(c).wait_recv()
        tpart(c).wait_recv()
        fill = jnp.zeros((tok - 2 * groups, HD), jnp.float32)
        theirs = jnp.transpose(jnp.concatenate([strecv[c], fill], axis=0))
        mine = stat[lax.rem(c, 2)]
        top = jnp.maximum(mine, theirs)
        for j in range(groups):
            a, b = slice(j, j + 1), slice(groups + j, groups + j + 1)
            wa = mine[:, b] * jnp.exp2((mine[:, a] - top[:, a]) * COEF)
            wb = theirs[:, b] * jnp.exp2((theirs[:, a] - top[:, a]) * COEF)
            r = 1.0 / (wa + wb)
            o = own[lax.rem(c, 2), j] * (wa * r) + orecv[c, j].astype(jnp.float32) * (wb * r)
            out[:, pl.ds(pl.multiple_of(c * qw + j * HD, HD), HD)] = o.astype(jnp.bfloat16)

    def attention(c, _):
        swap(c).wait_recv()
        all2(c, 0).wait_recv()
        scores(c)
        all2(c, 1).wait_recv()
        values(c, 0)
        tpart(c).start()
        opart(c).start()
        values(c, 1)

        @pl.when(c > 0)
        def _():
            combine(c - 1)

        return 0

    lax.fori_loop(0, KVH, attention, 0)
    combine(KVH - 1)
    for p in range(parts):
        all1(p).wait_send()

    def finish(c, _):
        swap(c).wait_send()
        all2(c, 0).wait_send()
        all2(c, 1).wait_send()
        opart(c).wait_send()
        tpart(c).wait_send()
        return 0

    lax.fori_loop(0, KVH, finish, 0)


def on_device(old_cache, block_table, place_after, context_len, queries, new_kv):
    ninst = lax.axis_size("inst")
    ngroup = lax.axis_size("group")
    slots, blk, width = old_cache.shape[1:]
    tok, qw = queries.shape
    per_inst = block_table.shape[1] // ninst
    reqs, nblk = block_table.shape
    ctx = per_inst * blk
    groups = qw // (KVH * HD)
    rows = groups * tok
    sides = ninst // 2
    bf, f32 = jnp.bfloat16, jnp.float32
    dma = pltpu.SemaphoreType.DMA
    return pl.pallas_call(
        functools.partial(body, ngroup, ninst),
        out_shape=jax.ShapeDtypeStruct((tok, qw), bf),
        in_specs=[pl.BlockSpec(memory_space=pl.ANY)] * 6,
        out_specs=pl.BlockSpec(memory_space=pltpu.VMEM),
        scratch_shapes=[
            *[pltpu.VMEM((slots, len(kinds), blk, HD), bf) for _, kinds in PARTS * 2],
            pltpu.VMEM((slots, blk, width), bf),
            pltpu.VMEM((reqs, nblk), jnp.int32),
            pltpu.VMEM((1, reqs), jnp.int32),
            pltpu.VMEM((1, reqs), jnp.int32),
            pltpu.VMEM((ngroup + 8, HD), jnp.int32),
            pltpu.SMEM((ngroup + 8, HD), jnp.int32),
            pltpu.VMEM((KVH, 2, sides - 1, ctx, HD), bf),
            pltpu.VMEM((KVH, 2, sides, ctx, HD), bf),
            pltpu.VMEM((2, tok, qw), bf),
            pltpu.VMEM((tok, 2 * KVH * HD), bf),
            pltpu.VMEM((2 * rows, 2 * HD), bf),
            pltpu.VMEM((sides, ctx, HD), bf),
            pltpu.VMEM((2, tok, HD), bf),
            pltpu.VMEM((sides, 2 * rows, ctx), f32),
            pltpu.VMEM((2 * rows, tok), f32),
            pltpu.VMEM((2 * rows, HD), f32),
            pltpu.VMEM((2, groups, tok, HD), f32),
            pltpu.VMEM((2, tok, HD), f32),
            pltpu.VMEM((KVH, groups, tok, HD), bf),
            pltpu.VMEM((KVH, groups, tok, HD), bf),
            pltpu.VMEM((KVH, 2 * groups, HD), f32),
            pltpu.VMEM((KVH, 2 * groups, HD), f32),
            dma((7,)), dma((len(PARTS),)), dma((len(PARTS),)), dma((KVH, 2)), dma((KVH, 2)),
            dma((KVH,)), dma((KVH,)), dma((KVH,)), dma((KVH,)), dma((KVH,)), dma((KVH,)),
        ],
        compiler_params=pltpu.CompilerParams(
            collective_id=0, has_side_effects=True, vmem_limit_bytes=VLIM * 1024 * 1024
        ),
    )(*(
        pltpu.with_memory_space_constraint(x, pltpu.HBM)
        for x in (block_table, place_after[None], context_len[None], old_cache, queries, new_kv)
    ))


def solution(mesh):
    return jax.shard_map(
        on_device,
        mesh=mesh,
        in_specs=(
            P("inst", "group", None, None),
            P(),
            P(),
            P(),
            P(("group", "inst"), None),
            P(("group", "inst"), None),
        ),
        out_specs=P(("group", "inst"), None),
        check_vma=False,
    )
```

```python
import functools

import jax
import jax.numpy as jnp
from jax import lax
from jax.experimental import pallas as pl
from jax.experimental.pallas import tpu as pltpu
from jax.sharding import PartitionSpec as P

KVH = 8
HD = 128
PARTS = [(0, (0,)), (0, (1,))] + [(c, (0, 1)) for c in range(1, KVH)]
EARLY = 4
VLIM = 46
BIG = -1e30
COEF = float(HD) ** -0.5 * 1.4426950408889634
MESH = pl.DeviceIdType.MESH


def onehot(cond):
    return jnp.where(cond, 1.0, 0.0).astype(jnp.bfloat16)


def tables(blocks, places, tab, g, i, ngroup, slots, items):
    reqs, nblk = blocks.shape
    rgroup = slots // items
    value = blocks[...]
    owner = (value // slots).astype(jnp.float32).astype(jnp.bfloat16)
    local = (value % slots).astype(jnp.float32).astype(jnp.bfloat16)
    k = lax.broadcasted_iota(jnp.int32, (nblk, HD), 0)
    lane = lax.broadcasted_iota(jnp.int32, (nblk, HD), 1)
    pick = onehot(k == i * items + lane % items)
    row = lax.broadcasted_iota(jnp.int32, (rgroup * ngroup, reqs), 0)
    place = row % ngroup * rgroup + row // ngroup
    order = onehot(jnp.broadcast_to(places[...], (rgroup * ngroup, reqs)) == place)

    def by_group(array):
        columns = jnp.dot(array, pick, preferred_element_type=jnp.float32).astype(jnp.bfloat16)
        rows = jnp.dot(order, columns, preferred_element_type=jnp.float32)
        within = lax.broadcasted_iota(jnp.int32, (ngroup, HD), 1) // items
        result = rows[:ngroup]
        for w in range(1, rgroup):
            result = jnp.where(within == w, rows[w * ngroup : (w + 1) * ngroup], result)
        return result.astype(jnp.int32)

    owners, locals_ = by_group(owner), by_group(local)
    item = lax.broadcasted_iota(jnp.int32, (ngroup, HD), 1)
    hit = (owners == g) & (item < slots)
    first = jnp.min(jnp.where(hit, item, HD), axis=1, keepdims=True)
    last = jnp.max(jnp.where(hit, item, -1), axis=1, keepdims=True)
    one = jnp.sum(jnp.where(item == first, locals_, 0), axis=1, keepdims=True)
    two = jnp.sum(jnp.where(item == last, locals_, 0), axis=1, keepdims=True)
    tab[:ngroup, :] = jnp.where(item == 0, one, two)
    mine = jnp.sum(
        jnp.where(lax.broadcasted_iota(jnp.int32, (ngroup, HD), 0) == g, owners, 0), axis=0, keepdims=True
    )
    across = jnp.broadcast_to(mine, (HD, HD)).astype(jnp.float32)
    down = jnp.transpose(across)
    t0 = lax.broadcasted_iota(jnp.int32, (HD, HD), 0)
    t1 = lax.broadcasted_iota(jnp.int32, (HD, HD), 1)
    before = jnp.sum(jnp.where((across == down) & (t0 < t1), 1, 0), axis=0, keepdims=True)
    per = slots // ngroup
    arrival = (g - mine + ngroup) % ngroup * per + jnp.minimum(before, per - 1)
    tab[ngroup:, :] = jnp.broadcast_to(arrival, (tab.shape[0] - ngroup, HD))


def body(ngroup, ninst, blocks_hbm, places_hbm, lengths_hbm, cache_hbm, q, kv, out, *scratch):
    parts = len(PARTS)
    s1, r1 = scratch[:parts], scratch[parts : 2 * parts]
    (cache, blocks, places, lengths, tab, tbl, s2, r2, qx, kvx, qs, kbias, fbias, sref, sfresh, mref, own, stat, oo, orecv, st, strecv,
     ld, s1sem, r1sem, s2sem, r2sem, xs, xr, osem, orsem, tsem, trsem) = scratch[2 * parts :]
    g = lax.axis_index("group")
    i = lax.axis_index("inst")
    slots, blk = cache.shape[:2]
    tok = q.shape[0]
    half = lax.rem(i, 2)
    sgn = 1 - 2 * half
    partner = i + sgn
    kw = KVH * HD
    groups = q.shape[1] // kw
    qw = groups * HD
    rows = groups * tok
    per = slots // ngroup
    items = slots // (ninst // 2)
    ctx = items * blk
    sides = ninst // 2

    pairs = [
        (blocks_hbm, blocks), (places_hbm, places), (lengths_hbm, lengths),
        (cache_hbm.at[0], cache), (kv, kvx), (q, qx.at[1]),
    ]
    loads = [pltpu.make_async_copy(src, dst, ld.at[n]) for n, (src, dst) in enumerate(pairs)]
    for copy in loads:
        copy.start()

    barrier = pltpu.get_barrier_semaphore()

    def greet_group(d, _):
        pl.semaphore_signal(barrier, inc=1, device_id=(lax.rem(g + d, ngroup), i), device_id_type=MESH)
        return 0

    def greet_inst(e, _):
        pl.semaphore_signal(barrier, inc=1, device_id=(g, lax.rem(i + e, ninst)), device_id_type=MESH)
        return 0

    lax.fori_loop(1, ngroup, greet_group, 0)
    lax.fori_loop(1, ninst, greet_inst, 0)


    def permute1(p):
        c, kinds = PARTS[p]

        def step(k, _):
            s = tbl[lax.rem(g + k // per, ngroup), lax.rem(k, per)]
            for n, t in enumerate(kinds):
                s1[p][k, n] = cache[s, :, t * kw + c * HD : t * kw + (c + 1) * HD]
            return 0

        lax.fori_loop(0, slots, step, 0, unroll=8)
        for k in range(per):
            r1[p][k] = s1[p][k]

    def send1(p):
        def step(d, _):
            pltpu.make_async_remote_copy(
                src_ref=s1[p].at[pl.ds(per * d, per)],
                dst_ref=r1[p].at[pl.ds(per * d, per)],
                send_sem=s1sem.at[p],
                recv_sem=r1sem.at[p],
                device_id=(lax.rem(g + d, ngroup), i),
                device_id_type=MESH,
            ).start()
            return 0

        lax.fori_loop(1, ngroup, step, 0)

    def all1(p):
        return pltpu.make_async_remote_copy(
            src_ref=s1[p].at[pl.ds(per, slots - per)],
            dst_ref=r1[p].at[pl.ds(per, slots - per)],
            send_sem=s1sem.at[p],
            recv_sem=r1sem.at[p],
            device_id=(lax.rem(g + 1, ngroup), i),
            device_id_type=MESH,
        )

    def target(n):
        step = (0, -1, 2, -3)[n]
        return lax.rem(i + sgn * step + ninst, ninst)

    def permute2(p):
        c, kinds = PARTS[p]
        for n in range(sides):
            base = target(n) // 2 * items

            def step(k, _):
                idx = tbl[ngroup, base + k]
                for m, t in enumerate(kinds):
                    if n == 0:
                        r2[c, t, 0, pl.ds(k * blk, blk), :] = r1[p][idx, m]
                    else:
                        s2[c, t, n - 1, pl.ds(k * blk, blk), :] = r1[p][idx, m]
                return 0

            lax.fori_loop(0, items, step, 0, unroll=8)

    def send2(c, t):
        for n in range(sides - 1, 0, -1):
            pltpu.make_async_remote_copy(
                src_ref=s2.at[c, t, n - 1],
                dst_ref=r2.at[c, t, n],
                send_sem=s2sem.at[c, t],
                recv_sem=r2sem.at[c, t],
                device_id=(g, target(n)),
                device_id_type=MESH,
            ).start()

    def all2(c, t):
        return pltpu.make_async_remote_copy(
            src_ref=s2.at[c, t],
            dst_ref=r2.at[c, t, pl.ds(1, sides - 1)],
            send_sem=s2sem.at[c, t],
            recv_sem=r2sem.at[c, t],
            device_id=(g, partner),
            device_id_type=MESH,
        )

    def to_partner(src, dst, ssem, rsem):
        return pltpu.make_async_remote_copy(
            src_ref=src, dst_ref=dst, send_sem=ssem, recv_sem=rsem,
            device_id=(g, partner), device_id_type=MESH,
        )

    def swap(c):
        cols = pl.ds(pl.multiple_of(c * qw, qw), qw)
        return to_partner(q.at[:, cols], qx.at[0, :, cols], xs.at[c], xr.at[c])

    for copy in loads[:3]:
        copy.wait()
    tables(blocks, places, tab, g, i, ngroup, slots, items)
    to_scalars = pltpu.make_async_copy(tab, tbl, ld.at[len(pairs)])
    to_scalars.start()
    loads[3].wait()
    to_scalars.wait()
    permute1(0)
    pl.semaphore_wait(barrier, ngroup - 1 + ninst - 1)
    send1(0)
    permute1(1)
    send1(1)
    for c in range(EARLY):
        swap(c).start()
    for p in range(2, parts):
        permute1(p)
        send1(p)

    slot = g * (slots // items) + i // 2
    length = jnp.sum(jnp.where(places[...] == slot, lengths[...], 0), axis=1, keepdims=True)
    eye = (
        lax.broadcasted_iota(jnp.int32, (tok, tok), 0)
        == lax.broadcasted_iota(jnp.int32, (tok, tok), 1)
    )
    for b in range(2 * groups):
        qs[pl.ds(b * tok, tok), HD:] = jnp.where(eye, 1.0, 0.0).astype(jnp.bfloat16)
    row = lax.broadcasted_iota(jnp.int32, (ctx, HD), 0)
    for n in range(sides):
        source = lax.rem(i - sgn * n + ninst, ninst)
        kbias[n] = jnp.where(row + source * ctx < length, 0.0, BIG).astype(jnp.bfloat16)
    key = lax.broadcasted_iota(jnp.int32, (tok, HD), 0)
    query = lax.broadcasted_iota(jnp.int32, (tok, HD), 1)
    flag = jnp.full((tok, HD), half, jnp.int32)
    fbias[0] = jnp.where(flag == 0, 0.0, BIG).astype(jnp.bfloat16)
    fbias[1] = jnp.where(key <= query, 0.0, BIG).astype(jnp.bfloat16)

    for p, (c, kinds) in enumerate(PARTS):
        all1(p).wait_recv()
        permute2(p)
        for t in kinds:
            send2(c, t)
        if 1 in kinds and c + EARLY < KVH:
            swap(c + EARLY).start()

    for copy in loads[4:]:
        copy.wait()

    nt = (((1,), (1,)), ((), ()))

    def score(qv, k, bias):
        return lax.dot_general(
            qv, jnp.concatenate([k, bias], axis=1), nt, preferred_element_type=jnp.float32
        )

    lane = lax.broadcasted_iota(jnp.int32, (tok, HD), 1)
    rb = 2 * tok
    ones = jnp.ones((ctx, HD), jnp.bfloat16)

    def opart(c, b):
        return to_partner(oo.at[c, b], orecv.at[c, b], osem.at[c, b], orsem.at[c, b])

    def tpart(c):
        return to_partner(st.at[c], strecv.at[c], tsem.at[c], trsem.at[c])

    def scores(c):
        for h in range(2):
            for j in range(groups):
                qs[pl.ds((h * groups + j) * tok, tok), :HD] = qx[
                    h, :, pl.ds(pl.multiple_of(c * qw + j * HD, HD), HD)
                ]
            span = pl.ds(h * rows, rows)
            s = score(qs[span, :], kvx[:, pl.ds(pl.multiple_of(c * HD, HD), HD)], fbias[h])
            sfresh[span, :] = s
            mref[span, :] = s

        def first(n, _):
            s = score(qs[...], r2[c, 0, n], kbias[n])
            sref[n] = s
            mref[...] = jnp.maximum(mref[...], jnp.maximum(s[:, :HD], s[:, HD:]))
            return 0

        lax.fori_loop(0, sides, first, 0)

    def values(c, h):
        vf = kvx[:, pl.ds(pl.multiple_of(kw + c * HD, HD), HD)]
        stats = jnp.zeros((tok, HD), jnp.float32)
        for b in range(rows // rb):
            span = pl.ds(h * rows + b * rb, rb)
            m = jnp.max(mref[span, :], axis=1, keepdims=True)
            total = jnp.dot(
                jnp.exp2((sfresh[span, :] - m) * COEF).astype(jnp.bfloat16),
                jnp.concatenate([vf, ones[:tok]], axis=1),
                preferred_element_type=jnp.float32,
            )
            for n in range(sides):
                w = jnp.exp2((sref[n, span, :] - m) * COEF).astype(jnp.bfloat16)
                total = total + jnp.dot(
                    w, jnp.concatenate([r2[c, 1, n], ones], axis=1), preferred_element_type=jnp.float32
                )
            o = total[:, :HD] / total[:, HD:]
            for j in range(rb // tok):
                at = b * (rb // tok) + j
                part = slice(j * tok, (j + 1) * tok)
                stats = jnp.where(lane == at, m[part], stats)
                stats = jnp.where(lane == groups + at, total[part, HD:], stats)
                if h == 1:
                    own[lax.rem(c, 2), at] = o[part]
                else:
                    oo[c, b, j] = o[part].astype(jnp.bfloat16)
            if h == 0 and b == 0:
                opart(c, 0).start()
        if h == 1:
            stat[lax.rem(c, 2)] = stats
        else:
            st[c] = jnp.transpose(stats)[: 2 * groups]

    def combine(c):
        tpart(c).wait_recv()
        fill = jnp.zeros((tok - 2 * groups, HD), jnp.float32)
        theirs = jnp.transpose(jnp.concatenate([strecv[c], fill], axis=0))
        mine = stat[lax.rem(c, 2)]
        top = jnp.maximum(mine, theirs)
        for j in range(groups):
            if j % 2 == 0:
                opart(c, j // 2).wait_recv()
            a, b = slice(j, j + 1), slice(groups + j, groups + j + 1)
            wa = mine[:, b] * jnp.exp2((mine[:, a] - top[:, a]) * COEF)
            wb = theirs[:, b] * jnp.exp2((theirs[:, a] - top[:, a]) * COEF)
            r = 1.0 / (wa + wb)
            o = own[lax.rem(c, 2), j] * (wa * r) + orecv[c, j // 2, j % 2].astype(jnp.float32) * (wb * r)
            out[:, pl.ds(pl.multiple_of(c * qw + j * HD, HD), HD)] = o.astype(jnp.bfloat16)

    def attention(c, _):
        swap(c).wait_recv()
        all2(c, 0).wait_recv()
        scores(c)
        all2(c, 1).wait_recv()
        values(c, 0)
        tpart(c).start()
        opart(c, 1).start()
        values(c, 1)

        @pl.when(c > 0)
        def _():
            combine(c - 1)

        return 0

    lax.fori_loop(0, KVH, attention, 0)
    combine(KVH - 1)
    for p in range(parts):
        all1(p).wait_send()

    def finish(c, _):
        swap(c).wait_send()
        all2(c, 0).wait_send()
        all2(c, 1).wait_send()
        opart(c, 0).wait_send()
        opart(c, 1).wait_send()
        tpart(c).wait_send()
        return 0

    lax.fori_loop(0, KVH, finish, 0)


def on_device(old_cache, block_table, place_after, context_len, queries, new_kv):
    ninst = lax.axis_size("inst")
    ngroup = lax.axis_size("group")
    slots, blk, width = old_cache.shape[1:]
    tok, qw = queries.shape
    per_inst = block_table.shape[1] // ninst
    reqs, nblk = block_table.shape
    ctx = per_inst * blk
    groups = qw // (KVH * HD)
    rows = groups * tok
    sides = ninst // 2
    bf, f32 = jnp.bfloat16, jnp.float32
    dma = pltpu.SemaphoreType.DMA
    return pl.pallas_call(
        functools.partial(body, ngroup, ninst),
        out_shape=jax.ShapeDtypeStruct((tok, qw), bf),
        in_specs=[pl.BlockSpec(memory_space=pl.ANY)] * 6,
        out_specs=pl.BlockSpec(memory_space=pltpu.VMEM),
        scratch_shapes=[
            *[pltpu.VMEM((slots, len(kinds), blk, HD), bf) for _, kinds in PARTS * 2],
            pltpu.VMEM((slots, blk, width), bf),
            pltpu.VMEM((reqs, nblk), jnp.int32),
            pltpu.VMEM((1, reqs), jnp.int32),
            pltpu.VMEM((1, reqs), jnp.int32),
            pltpu.VMEM((ngroup + 8, HD), jnp.int32),
            pltpu.SMEM((ngroup + 8, HD), jnp.int32),
            pltpu.VMEM((KVH, 2, sides - 1, ctx, HD), bf),
            pltpu.VMEM((KVH, 2, sides, ctx, HD), bf),
            pltpu.VMEM((2, tok, qw), bf),
            pltpu.VMEM((tok, 2 * KVH * HD), bf),
            pltpu.VMEM((2 * rows, 2 * HD), bf),
            pltpu.VMEM((sides, ctx, HD), bf),
            pltpu.VMEM((2, tok, HD), bf),
            pltpu.VMEM((sides, 2 * rows, ctx), f32),
            pltpu.VMEM((2 * rows, tok), f32),
            pltpu.VMEM((2 * rows, HD), f32),
            pltpu.VMEM((2, groups, tok, HD), f32),
            pltpu.VMEM((2, tok, HD), f32),
            pltpu.VMEM((KVH, 2, groups // 2, tok, HD), bf),
            pltpu.VMEM((KVH, 2, groups // 2, tok, HD), bf),
            pltpu.VMEM((KVH, 2 * groups, HD), f32),
            pltpu.VMEM((KVH, 2 * groups, HD), f32),
            dma((7,)), dma((len(PARTS),)), dma((len(PARTS),)), dma((KVH, 2)), dma((KVH, 2)),
            dma((KVH,)), dma((KVH,)), dma((KVH, 2)), dma((KVH, 2)), dma((KVH,)), dma((KVH,)),
        ],
        compiler_params=pltpu.CompilerParams(
            collective_id=0, has_side_effects=True, vmem_limit_bytes=VLIM * 1024 * 1024
        ),
    )(*(
        pltpu.with_memory_space_constraint(x, pltpu.HBM)
        for x in (block_table, place_after[None], context_len[None], old_cache, queries, new_kv)
    ))


def solution(mesh):
    return jax.shard_map(
        on_device,
        mesh=mesh,
        in_specs=(
            P("inst", "group", None, None),
            P(),
            P(),
            P(),
            P(("group", "inst"), None),
            P(("group", "inst"), None),
        ),
        out_specs=P(("group", "inst"), None),
        check_vma=False,
    )
```

```python
import functools

import jax
import jax.numpy as jnp
from jax import lax
from jax.experimental import pallas as pl
from jax.experimental.pallas import tpu as pltpu
from jax.sharding import PartitionSpec as P

KVH = 8
HD = 128
PARTS = [(0, (0,)), (0, (1,))] + [(c, (0, 1)) for c in range(1, KVH)]
EARLY = 4
VLIM = 46
BIG = -1e30
COEF = float(HD) ** -0.5 * 1.4426950408889634
MESH = pl.DeviceIdType.MESH


def onehot(cond):
    return jnp.where(cond, 1.0, 0.0).astype(jnp.bfloat16)


def tables(blocks, places, tab, g, i, ngroup, slots, items):
    reqs, nblk = blocks.shape
    rgroup = slots // items
    value = blocks[...]
    owner = (value // slots).astype(jnp.float32).astype(jnp.bfloat16)
    local = (value % slots).astype(jnp.float32).astype(jnp.bfloat16)
    k = lax.broadcasted_iota(jnp.int32, (nblk, HD), 0)
    lane = lax.broadcasted_iota(jnp.int32, (nblk, HD), 1)
    pick = onehot(k == i * items + lane % items)
    row = lax.broadcasted_iota(jnp.int32, (rgroup * ngroup, reqs), 0)
    place = row % ngroup * rgroup + row // ngroup
    order = onehot(jnp.broadcast_to(places[...], (rgroup * ngroup, reqs)) == place)

    def by_group(array):
        columns = jnp.dot(array, pick, preferred_element_type=jnp.float32).astype(jnp.bfloat16)
        rows = jnp.dot(order, columns, preferred_element_type=jnp.float32)
        within = lax.broadcasted_iota(jnp.int32, (ngroup, HD), 1) // items
        result = rows[:ngroup]
        for w in range(1, rgroup):
            result = jnp.where(within == w, rows[w * ngroup : (w + 1) * ngroup], result)
        return result.astype(jnp.int32)

    owners, locals_ = by_group(owner), by_group(local)
    item = lax.broadcasted_iota(jnp.int32, (ngroup, HD), 1)
    hit = (owners == g) & (item < slots)
    first = jnp.min(jnp.where(hit, item, HD), axis=1, keepdims=True)
    last = jnp.max(jnp.where(hit, item, -1), axis=1, keepdims=True)
    one = jnp.sum(jnp.where(item == first, locals_, 0), axis=1, keepdims=True)
    two = jnp.sum(jnp.where(item == last, locals_, 0), axis=1, keepdims=True)
    tab[:ngroup, :] = jnp.where(item == 0, one, two)
    mine = jnp.sum(
        jnp.where(lax.broadcasted_iota(jnp.int32, (ngroup, HD), 0) == g, owners, 0), axis=0, keepdims=True
    )
    across = jnp.broadcast_to(mine, (HD, HD)).astype(jnp.float32)
    down = jnp.transpose(across)
    t0 = lax.broadcasted_iota(jnp.int32, (HD, HD), 0)
    t1 = lax.broadcasted_iota(jnp.int32, (HD, HD), 1)
    before = jnp.sum(jnp.where((across == down) & (t0 < t1), 1, 0), axis=0, keepdims=True)
    per = slots // ngroup
    arrival = (g - mine + ngroup) % ngroup * per + jnp.minimum(before, per - 1)
    tab[ngroup:, :] = jnp.broadcast_to(arrival, (tab.shape[0] - ngroup, HD))


def body(ngroup, ninst, blocks_hbm, places_hbm, lengths_hbm, cache_hbm, q, kv, out, *scratch):
    parts = len(PARTS)
    s1, r1 = scratch[:parts], scratch[parts : 2 * parts]
    (cache, blocks, places, lengths, tab, tbl, s2, r2, qx, kvx, qs, kbias, fbias, sref, sfresh, mref, own, stat, oo, orecv, st, strecv,
     ld, s1sem, r1sem, s2sem, r2sem, xs, xr, osem, orsem, tsem, trsem) = scratch[2 * parts :]
    g = lax.axis_index("group")
    i = lax.axis_index("inst")
    slots, blk = cache.shape[:2]
    tok = q.shape[0]
    half = lax.rem(i, 2)
    sgn = 1 - 2 * half
    partner = i + sgn
    kw = KVH * HD
    groups = q.shape[1] // kw
    qw = groups * HD
    rows = groups * tok
    per = slots // ngroup
    items = slots // (ninst // 2)
    ctx = items * blk
    sides = ninst // 2

    pairs = [
        (blocks_hbm, blocks), (places_hbm, places), (lengths_hbm, lengths),
        (cache_hbm.at[0], cache), (kv, kvx), (q, qx.at[1]),
    ]
    loads = [pltpu.make_async_copy(src, dst, ld.at[n]) for n, (src, dst) in enumerate(pairs)]
    for copy in loads:
        copy.start()

    barrier = pltpu.get_barrier_semaphore()

    def greet_group(d, _):
        pl.semaphore_signal(barrier, inc=1, device_id=(lax.rem(g + d, ngroup), i), device_id_type=MESH)
        return 0

    def greet_inst(e, _):
        pl.semaphore_signal(barrier, inc=1, device_id=(g, lax.rem(i + e, ninst)), device_id_type=MESH)
        return 0

    lax.fori_loop(1, ngroup, greet_group, 0)
    lax.fori_loop(1, ninst, greet_inst, 0)


    def permute1(p):
        c, kinds = PARTS[p]

        def step(k, _):
            s = tbl[lax.rem(g + k // per, ngroup), lax.rem(k, per)]
            for n, t in enumerate(kinds):
                s1[p][k, n] = cache[s, :, t * kw + c * HD : t * kw + (c + 1) * HD]
            return 0

        lax.fori_loop(0, slots, step, 0, unroll=8)
        for k in range(per):
            r1[p][k] = s1[p][k]

    def send1(p):
        def step(d, _):
            pltpu.make_async_remote_copy(
                src_ref=s1[p].at[pl.ds(per * d, per)],
                dst_ref=r1[p].at[pl.ds(per * d, per)],
                send_sem=s1sem.at[p],
                recv_sem=r1sem.at[p],
                device_id=(lax.rem(g + d, ngroup), i),
                device_id_type=MESH,
            ).start()
            return 0

        lax.fori_loop(1, ngroup, step, 0)

    def all1(p):
        return pltpu.make_async_remote_copy(
            src_ref=s1[p].at[pl.ds(per, slots - per)],
            dst_ref=r1[p].at[pl.ds(per, slots - per)],
            send_sem=s1sem.at[p],
            recv_sem=r1sem.at[p],
            device_id=(lax.rem(g + 1, ngroup), i),
            device_id_type=MESH,
        )

    def target(n):
        step = (0, -1, 2, -3)[n]
        return lax.rem(i + sgn * step + ninst, ninst)

    def permute2(p):
        c, kinds = PARTS[p]
        for n in range(sides):
            base = target(n) // 2 * items

            def step(k, _):
                idx = tbl[ngroup, base + k]
                for m, t in enumerate(kinds):
                    if n == 0:
                        r2[c, t, 0, pl.ds(k * blk, blk), :] = r1[p][idx, m]
                    else:
                        s2[c, t, n - 1, pl.ds(k * blk, blk), :] = r1[p][idx, m]
                return 0

            lax.fori_loop(0, items, step, 0, unroll=8)

    def send2(c, t):
        for n in range(sides - 1, 0, -1):
            pltpu.make_async_remote_copy(
                src_ref=s2.at[c, t, n - 1],
                dst_ref=r2.at[c, t, n],
                send_sem=s2sem.at[c, t],
                recv_sem=r2sem.at[c, t],
                device_id=(g, target(n)),
                device_id_type=MESH,
            ).start()

    def all2(c, t):
        return pltpu.make_async_remote_copy(
            src_ref=s2.at[c, t],
            dst_ref=r2.at[c, t, pl.ds(1, sides - 1)],
            send_sem=s2sem.at[c, t],
            recv_sem=r2sem.at[c, t],
            device_id=(g, partner),
            device_id_type=MESH,
        )

    def to_partner(src, dst, ssem, rsem):
        return pltpu.make_async_remote_copy(
            src_ref=src, dst_ref=dst, send_sem=ssem, recv_sem=rsem,
            device_id=(g, partner), device_id_type=MESH,
        )

    def swap(c):
        cols = pl.ds(pl.multiple_of(c * qw, qw), qw)
        return to_partner(q.at[:, cols], qx.at[0, :, cols], xs.at[c], xr.at[c])

    for copy in loads[:3]:
        copy.wait()
    tables(blocks, places, tab, g, i, ngroup, slots, items)
    to_scalars = pltpu.make_async_copy(tab, tbl, ld.at[len(pairs)])
    to_scalars.start()
    loads[3].wait()
    to_scalars.wait()
    permute1(0)
    pl.semaphore_wait(barrier, ngroup - 1 + ninst - 1)
    send1(0)
    permute1(1)
    send1(1)
    for c in range(EARLY):
        swap(c).start()
    for p in range(2, parts):
        permute1(p)
        send1(p)

    slot = g * (slots // items) + i // 2
    length = jnp.sum(jnp.where(places[...] == slot, lengths[...], 0), axis=1, keepdims=True)
    eye = (
        lax.broadcasted_iota(jnp.int32, (tok, tok), 0)
        == lax.broadcasted_iota(jnp.int32, (tok, tok), 1)
    )
    for b in range(2 * groups):
        qs[pl.ds(b * tok, tok), HD:] = jnp.where(eye, 1.0, 0.0).astype(jnp.bfloat16)
    row = lax.broadcasted_iota(jnp.int32, (ctx, HD), 0)
    for n in range(sides):
        source = lax.rem(i - sgn * n + ninst, ninst)
        kbias[n] = jnp.where(row + source * ctx < length, 0.0, BIG).astype(jnp.bfloat16)
    key = lax.broadcasted_iota(jnp.int32, (tok, HD), 0)
    query = lax.broadcasted_iota(jnp.int32, (tok, HD), 1)
    flag = jnp.full((tok, HD), half, jnp.int32)
    fbias[0] = jnp.where(flag == 0, 0.0, BIG).astype(jnp.bfloat16)
    fbias[1] = jnp.where(key <= query, 0.0, BIG).astype(jnp.bfloat16)

    for p, (c, kinds) in enumerate(PARTS):
        all1(p).wait_recv()
        permute2(p)
        for t in kinds:
            send2(c, t)
        if 1 in kinds and c + EARLY < KVH:
            swap(c + EARLY).start()

    for copy in loads[4:]:
        copy.wait()

    nt = (((1,), (1,)), ((), ()))

    def score(qv, k, bias):
        return lax.dot_general(
            qv, jnp.concatenate([k, bias], axis=1), nt, preferred_element_type=jnp.float32
        )

    lane = lax.broadcasted_iota(jnp.int32, (tok, HD), 1)
    rb = 2 * tok
    ones = jnp.ones((ctx, HD), jnp.bfloat16)

    def opart(c, b):
        return to_partner(oo.at[c, b], orecv.at[c, b], osem.at[c, b], orsem.at[c, b])

    def tpart(c):
        return to_partner(st.at[c], strecv.at[c], tsem.at[c], trsem.at[c])

    def scores(c):
        for h in range(2):
            for j in range(groups):
                qs[pl.ds((h * groups + j) * tok, tok), :HD] = qx[
                    h, :, pl.ds(pl.multiple_of(c * qw + j * HD, HD), HD)
                ]
            span = pl.ds(h * rows, rows)
            s = score(qs[span, :], kvx[:, pl.ds(pl.multiple_of(c * HD, HD), HD)], fbias[h])
            sfresh[span, :] = s
            mref[span, :] = s

        def first(n, _):
            s = score(qs[...], r2[c, 0, n], kbias[n])
            sref[n] = s
            mref[...] = jnp.maximum(mref[...], jnp.maximum(s[:, :HD], s[:, HD:]))
            return 0

        lax.fori_loop(0, sides, first, 0)

    def values(c, h):
        vf = kvx[:, pl.ds(pl.multiple_of(kw + c * HD, HD), HD)]
        stats = jnp.zeros((tok, HD), jnp.float32)
        for b in range(rows // rb):
            span = pl.ds(h * rows + b * rb, rb)
            m = jnp.max(mref[span, :], axis=1, keepdims=True)
            total = jnp.dot(
                jnp.exp2((sfresh[span, :] - m) * COEF).astype(jnp.bfloat16),
                jnp.concatenate([vf, ones[:tok]], axis=1),
                preferred_element_type=jnp.float32,
            )
            for n in range(sides):
                w = jnp.exp2((sref[n, span, :] - m) * COEF).astype(jnp.bfloat16)
                total = total + jnp.dot(
                    w, jnp.concatenate([r2[c, 1, n], ones], axis=1), preferred_element_type=jnp.float32
                )
            o = total[:, :HD] / total[:, HD:]
            for j in range(rb // tok):
                at = b * (rb // tok) + j
                part = slice(j * tok, (j + 1) * tok)
                stats = jnp.where(lane == at, m[part], stats)
                stats = jnp.where(lane == groups + at, total[part, HD:], stats)
                if h == 1:
                    own[lax.rem(c, 2), at] = o[part]
                else:
                    oo[c, b, j] = o[part].astype(jnp.bfloat16)
            if h == 0 and b == 0:
                opart(c, 0).start()
        if h == 1:
            stat[lax.rem(c, 2)] = stats
        else:
            st[c] = jnp.transpose(stats)[: 2 * groups]

    def combine(c):
        tpart(c).wait_recv()
        fill = jnp.zeros((tok - 2 * groups, HD), jnp.float32)
        theirs = jnp.transpose(jnp.concatenate([strecv[c], fill], axis=0))
        mine = stat[lax.rem(c, 2)]
        top = jnp.maximum(mine, theirs)
        for j in range(groups):
            if j % 2 == 0:
                opart(c, j // 2).wait_recv()
            a, b = slice(j, j + 1), slice(groups + j, groups + j + 1)
            wa = mine[:, b] * jnp.exp2((mine[:, a] - top[:, a]) * COEF)
            wb = theirs[:, b] * jnp.exp2((theirs[:, a] - top[:, a]) * COEF)
            r = 1.0 / (wa + wb)
            o = own[lax.rem(c, 2), j] * (wa * r) + orecv[c, j // 2, j % 2].astype(jnp.float32) * (wb * r)
            out[:, pl.ds(pl.multiple_of(c * qw + j * HD, HD), HD)] = o.astype(jnp.bfloat16)

    def attention(c, _):
        swap(c).wait_recv()
        all2(c, 0).wait_recv()
        scores(c)
        all2(c, 1).wait_recv()
        values(c, 0)
        tpart(c).start()
        opart(c, 1).start()
        values(c, 1)

        @pl.when(c > 0)
        def _():
            combine(c - 1)

        return 0

    lax.fori_loop(0, KVH, attention, 0)
    for p in range(parts):
        all1(p).wait_send()

    def finish(c, _):
        swap(c).wait_send()
        all2(c, 0).wait_send()
        all2(c, 1).wait_send()
        tpart(c).wait_send()
        return 0

    lax.fori_loop(0, KVH, finish, 0)
    combine(KVH - 1)

    def finish_parts(c, _):
        opart(c, 0).wait_send()
        opart(c, 1).wait_send()
        return 0

    lax.fori_loop(0, KVH, finish_parts, 0)


def on_device(old_cache, block_table, place_after, context_len, queries, new_kv):
    ninst = lax.axis_size("inst")
    ngroup = lax.axis_size("group")
    slots, blk, width = old_cache.shape[1:]
    tok, qw = queries.shape
    per_inst = block_table.shape[1] // ninst
    reqs, nblk = block_table.shape
    ctx = per_inst * blk
    groups = qw // (KVH * HD)
    rows = groups * tok
    sides = ninst // 2
    bf, f32 = jnp.bfloat16, jnp.float32
    dma = pltpu.SemaphoreType.DMA
    return pl.pallas_call(
        functools.partial(body, ngroup, ninst),
        out_shape=jax.ShapeDtypeStruct((tok, qw), bf),
        in_specs=[pl.BlockSpec(memory_space=pl.ANY)] * 6,
        out_specs=pl.BlockSpec(memory_space=pltpu.VMEM),
        scratch_shapes=[
            *[pltpu.VMEM((slots, len(kinds), blk, HD), bf) for _, kinds in PARTS * 2],
            pltpu.VMEM((slots, blk, width), bf),
            pltpu.VMEM((reqs, nblk), jnp.int32),
            pltpu.VMEM((1, reqs), jnp.int32),
            pltpu.VMEM((1, reqs), jnp.int32),
            pltpu.VMEM((ngroup + 8, HD), jnp.int32),
            pltpu.SMEM((ngroup + 8, HD), jnp.int32),
            pltpu.VMEM((KVH, 2, sides - 1, ctx, HD), bf),
            pltpu.VMEM((KVH, 2, sides, ctx, HD), bf),
            pltpu.VMEM((2, tok, qw), bf),
            pltpu.VMEM((tok, 2 * KVH * HD), bf),
            pltpu.VMEM((2 * rows, 2 * HD), bf),
            pltpu.VMEM((sides, ctx, HD), bf),
            pltpu.VMEM((2, tok, HD), bf),
            pltpu.VMEM((sides, 2 * rows, ctx), f32),
            pltpu.VMEM((2 * rows, tok), f32),
            pltpu.VMEM((2 * rows, HD), f32),
            pltpu.VMEM((2, groups, tok, HD), f32),
            pltpu.VMEM((2, tok, HD), f32),
            pltpu.VMEM((KVH, 2, groups // 2, tok, HD), bf),
            pltpu.VMEM((KVH, 2, groups // 2, tok, HD), bf),
            pltpu.VMEM((KVH, 2 * groups, HD), f32),
            pltpu.VMEM((KVH, 2 * groups, HD), f32),
            dma((7,)), dma((len(PARTS),)), dma((len(PARTS),)), dma((KVH, 2)), dma((KVH, 2)),
            dma((KVH,)), dma((KVH,)), dma((KVH, 2)), dma((KVH, 2)), dma((KVH,)), dma((KVH,)),
        ],
        compiler_params=pltpu.CompilerParams(
            collective_id=0, has_side_effects=True, vmem_limit_bytes=VLIM * 1024 * 1024
        ),
    )(*(
        pltpu.with_memory_space_constraint(x, pltpu.HBM)
        for x in (block_table, place_after[None], context_len[None], old_cache, queries, new_kv)
    ))


def solution(mesh):
    return jax.shard_map(
        on_device,
        mesh=mesh,
        in_specs=(
            P("inst", "group", None, None),
            P(),
            P(),
            P(),
            P(("group", "inst"), None),
            P(("group", "inst"), None),
        ),
        out_specs=P(("group", "inst"), None),
        check_vma=False,
    )
```
